32 devices in a mesh: row: 8 (over z, x), col: 4 (over y, core).
Axes of the slice: x: 2, y: 2, z: 4, core: 2. Of those that a mesh axis runs over, the one named last changes fastest.
Arguments:
- spikes: int32 [10, 4096], P(None, ('row', 'col')), may hold values 0 or 1
- stp_init: float32 [2, 4096], P(None, ('row', 'col')), may hold values from 0.2 to 1
- trace_init: float32 [3, 4096], P(None, ('row', 'col')), may hold values from 0 to 1.5
- weights: float32 [8, 4, 256, 128, 128], P('row', 'col'), may hold values from 0 to 1
- block_pre: int32 [8, 4, 256], P('row', 'col'), may hold values from 0 to 7
- block_post: int32 [8, 4, 256], P('row', 'col'), may hold values from 0 to 3
- block_count: int32 [8, 4], P('row', 'col'), may hold values from 1 to 255, as said below
Outputs:
- new_weights: float32 [8, 4, 128, 128, 128], P('row', 'col')
- synaptic: float32 [10, 4096], P(None, ('row', 'col'))
The draws below stay inside these ranges and needn't reach their ends.
Inputs may be any that keep to these rules, and one draw needn't show every extreme that they name: block_count[r, c] + block_count[(r + 4) mod 8, c] = 256; some device uses 2 * 128 - 1 slots in every draw.
All inputs are finite; a program needn't handle non-finite values. No bound on the sum of `spikes` on one device may be relied on, other than what follows from the above.
Results may differ from the reference program's by a relative error of at most 0.0003.
Values sent between devices are 32-bit elements; how exact they have to be, the bound alone decides.
No kernel may reach another device: no remote copies, remote signals or barrier semaphores. Data moves between devices by JAX's collectives and lax.ppermute only.
A program may use at most 128 MiB of HBM per device.

```python
import math
import jax
import jax.numpy as jnp
import numpy as np
from jax import lax

GRP = 128
BLK_DEV = 128
STEPS = 10
SLOTS = 256
NEURONS = 4096
N_ROW = 8
N_COL = 4


def draw_block_count(key, part):
    half_rows = N_ROW // 2
    keys = jax.random.split(key, 5)
    first = jax.random.randint(keys[0], (half_rows, N_COL), 0, BLK_DEV)
    second = jax.random.randint(keys[1], (half_rows, N_COL), 0, BLK_DEV)
    spread_size = first * second // max(BLK_DEV - 1, 1)
    chosen_row = jax.random.randint(keys[2], (), 0, half_rows)
    chosen_col = jax.random.randint(keys[3], (), 0, N_COL)
    forced = (jnp.arange(half_rows)[:, None] == chosen_row) & (jnp.arange(N_COL)[None, :] == chosen_col)
    spread_size = jnp.where(forced, BLK_DEV - 1, spread_size)
    flips = jax.random.randint(keys[4], (half_rows, N_COL), 0, 2) * 2 - 1
    offset = spread_size * flips
    return jnp.concatenate([BLK_DEV + offset, BLK_DEV - offset], axis=0).astype(jnp.int32)


def touch_ends(entries, rng, smallest, largest):
    spot = [jax.random.randint(jax.random.fold_in(rng, axis), (), 0, length) for axis, length in enumerate(entries.shape)]
    main_axis = entries.shape.index(max(entries.shape))
    next_to = spot[:main_axis] + [(spot[main_axis] + 1) % entries.shape[main_axis]] + spot[main_axis + 1:]
    return entries.at[tuple(spot)].set(smallest).at[tuple(next_to)].set(largest)


def steps_of(stream_key, shape, shards, low, top_value):
    def one(dim, blocks):
        steps = jax.random.uniform(jax.random.fold_in(jax.random.fold_in(stream_key, 6), dim), (blocks,), jnp.float32, low / len(shards), top_value / len(shards))
        return jnp.repeat(jnp.exp(steps), shape[dim] // blocks).reshape((-1,) + (1,) * (len(shape) - dim - 1))

    loudness = one(*shards[0])
    for cut in shards[1:]:
        loudness = loudness * one(*cut)
    return loudness


def rank_table(amount, lean):
    weights = [(1 << 20) // math.isqrt(grade ** lean) + 1 for grade in range(1, amount + 1)]
    spread = 1 + sum(weights) // (1 << 30)
    return np.cumsum(np.array([max(1, weight // spread) for weight in weights]))


def skewed_ids(stream_key, extent, count, slope):
    grid = rank_table(count, slope)
    lot = jax.random.randint(jax.random.fold_in(stream_key, 1), extent, 0, int(grid[count - 1]))
    rank = jnp.searchsorted(jnp.asarray(grid, jnp.int32), lot, side="right")
    return jax.random.permutation(jax.random.fold_in(stream_key, 2), count)[rank].astype(jnp.int32)


def setup_inputs(seed: int = 0) -> dict:
    key_of = jax.random.split(jax.random.key(seed), 8)
    spikes = touch_ends((jax.random.randint(key_of[0], (STEPS, NEURONS), 0, 4) < 1).astype(jnp.int32), jax.random.fold_in(key_of[0], 1), 0, 1)
    stp_init = jnp.clip(0.2 + 0.8 * jax.random.uniform(key_of[1], (2, NEURONS), jnp.float32) ** steps_of(key_of[1], (2, NEURONS), ((1, 32),), -0.2, 0.2), 0.2, 1.0)
    trace_init = jnp.clip(1.5 * jax.random.uniform(key_of[2], (3, NEURONS), jnp.float32) ** steps_of(key_of[2], (3, NEURONS), ((1, 32),), -0.2, 0.2), 0.0, 1.5)
    weights = jnp.clip(1.0 * jax.random.uniform(key_of[3], (N_ROW, N_COL, SLOTS, GRP, GRP), jnp.float32) ** steps_of(key_of[3], (N_ROW, N_COL, SLOTS, GRP, GRP), ((0, 8), (1, 4)), -0.2, 0.2), 0.0, 1.0)
    block_pre = touch_ends(skewed_ids(key_of[4], (N_ROW, N_COL, SLOTS), N_ROW, 2), jax.random.fold_in(key_of[4], 3), 0, N_ROW - 1).astype(jnp.int32)
    block_post = touch_ends(jax.random.randint(key_of[5], (N_ROW, N_COL, SLOTS), 0, N_COL), jax.random.fold_in(key_of[5], 1), 0, N_COL - 1).astype(jnp.int32)
    block_count = draw_block_count(jax.random.fold_in(key_of[7], 71), 0)
    return dict(spikes=spikes, stp_init=stp_init, trace_init=trace_init, weights=weights, block_pre=block_pre, block_post=block_post, block_count=block_count)


HIGHEST = lax.Precision.HIGHEST
BASE_USE = 0.25
USE_DECAY = 0.98
SUPPLY_RATE = 0.005
PLUS_DECAY = math.exp(-1.0 / 16.8)
MINUS_DECAY = math.exp(-1.0 / 33.7)
SLOW_DECAY = math.exp(-1.0 / 114.0)
SYN_DECAY = math.exp(-1.0 / 5.0)
PAIR_UP = 1.0
TRIPLET_UP = 0.8
PAIR_DOWN = 0.9
LEARN_RATE = 0.02
WEIGHT_MAX = 1.0
INHIB_GAIN = 4.0

def neuron_traces(spikes, stp_init, trace_init):
    fired = spikes.astype(jnp.float32)

    def advance(carry, fired_now):
        use_level, supply, pre_fast, post_fast, post_slow = carry
        use_level = BASE_USE + (use_level - BASE_USE) * USE_DECAY
        use_level = use_level + fired_now * BASE_USE * (1.0 - use_level)
        release = fired_now * use_level * supply
        supply = supply + SUPPLY_RATE * (1.0 - supply) - release
        pre_fast = pre_fast * PLUS_DECAY + fired_now
        potent = fired_now * (PAIR_UP + TRIPLET_UP * post_slow)
        depress = PAIR_DOWN * post_fast
        post_fast = post_fast * MINUS_DECAY + fired_now
        post_slow = post_slow * SLOW_DECAY + fired_now
        return ((use_level, supply, pre_fast, post_fast, post_slow), (release, pre_fast, potent, depress))
    start = (stp_init[0], stp_init[1], trace_init[0], trace_init[1], trace_init[2])
    _, results = lax.scan(advance, start, fired)
    return results

def block_work(weights, pre_blocks, post_blocks, polarity):
    release = pre_blocks[:, 0]
    pre_fast = pre_blocks[:, 1]
    potent = post_blocks[:, 0]
    depress = post_blocks[:, 1]
    driven = release * polarity
    current = jnp.einsum('nij,nsj->nsi', weights, driven, precision=HIGHEST)
    post_terms = jnp.concatenate([potent, -depress], axis=1)
    pre_terms = jnp.concatenate([pre_fast, release], axis=1)
    change = jnp.einsum('nki,nkj->nij', post_terms, pre_terms, precision=HIGHEST)
    return (current, jnp.clip(weights + LEARN_RATE * change, 0.0, WEIGHT_MAX))

def arrange(own_updated, partner_upper, filled):
    half_slots = partner_upper.shape[0]
    places = jnp.arange(half_slots, dtype=jnp.int32)
    picked = jnp.clip(places - filled, 0, half_slots - 1).astype(jnp.int32)
    return jnp.where((places < filled)[:, None, None], own_updated[:half_slots], jnp.take(partner_upper, picked, axis=0))

def filtered(drive, gain):

    def advance(state, current):
        state = state * SYN_DECAY + gain * current
        return (state, state)
    _, result = lax.scan(advance, jnp.zeros_like(drive[0]), drive)
    return result

def reference(spikes, stp_init, trace_init, weights, block_pre, block_post, block_count):
    polarity = jnp.where(jnp.arange(GRP) % 5 == 4, -INHIB_GAIN, 1.0).astype(jnp.float32)
    release, pre_fast, potent, depress = neuron_traces(spikes, stp_init, trace_init)
    packed = jnp.stack([release, pre_fast, potent, depress]).reshape(4, STEPS, N_ROW, N_COL, GRP)
    pre_tables = jnp.transpose(packed[0:2], (3, 2, 0, 1, 4))
    post_all = packed[2:4]
    half_rows = N_ROW // 2

    def row_work(row_index, weights_row, pre_row, post_row, count_row):
        post_table = jnp.transpose(lax.dynamic_index_in_dim(post_all, row_index, 2, keepdims=False), (2, 0, 1, 3))

        def per_col(weights_col, pre_col, post_col, filled, pre_table):
            current, updated = block_work(weights_col, jnp.take(pre_table, pre_col, axis=0), jnp.take(post_table, post_col, axis=0), polarity)
            usable = jnp.arange(weights_col.shape[0], dtype=jnp.int32) < filled
            onehot = ((post_col[:, None] == jnp.arange(N_COL, dtype=jnp.int32)[None, :]) & usable[:, None]).astype(jnp.float32)
            return (jnp.einsum('nq,nsi->qsi', onehot, current, precision=HIGHEST), updated)
        partial_value, updated = jax.vmap(per_col)(weights_row, pre_row, post_row, count_row, pre_tables)
        return (lax.optimization_barrier(jnp.sum(partial_value, axis=0)), updated)

    def pair_work(items):
        row_low, low_weights, high_weights, low_pre, high_pre, low_post, high_post, low_count, high_count = items
        cur_low, upd_low = row_work(row_low, low_weights, low_pre, low_post, low_count)
        cur_high, upd_high = row_work(row_low + half_rows, high_weights, high_pre, high_post, high_count)
        new_low = jax.vmap(arrange)(upd_low, upd_high[:, BLK_DEV:], low_count)
        new_high = jax.vmap(arrange)(upd_high, upd_low[:, BLK_DEV:], high_count)
        return (cur_low, cur_high, new_low, new_high)
    cur_low, cur_high, new_low, new_high = lax.map(pair_work, (jnp.arange(half_rows, dtype=jnp.int32), weights[:half_rows], weights[half_rows:], block_pre[:half_rows], block_pre[half_rows:], block_post[:half_rows], block_post[half_rows:], block_count[:half_rows], block_count[half_rows:]))
    new_weights = jnp.concatenate([new_low, new_high], axis=0)
    drive = jnp.concatenate([cur_low, cur_high], axis=0)
    drive = jnp.transpose(drive, (2, 0, 1, 3)).reshape(STEPS, N_ROW * N_COL * GRP)
    synaptic = filtered(drive, 1.0 / math.sqrt(GRP * BLK_DEV))
    return (new_weights, synaptic)
```

```python
import math

import jax
import jax.numpy as jnp
from jax import lax
from jax.experimental import pallas as pl
from jax.experimental.pallas import tpu as pltpu
from jax.sharding import PartitionSpec as P

BASE_USE = 0.25
USE_DECAY = 0.98
SUPPLY_RATE = 0.005
PLUS_DECAY = math.exp(-1.0 / 16.8)
MINUS_DECAY = math.exp(-1.0 / 33.7)
SLOW_DECAY = math.exp(-1.0 / 114.0)
SYN_DECAY = math.exp(-1.0 / 5.0)
PAIR_UP = 1.0
TRIPLET_UP = 0.8
PAIR_DOWN = 0.9
LEARN_RATE = 0.02
WEIGHT_MAX = 1.0
INHIB_GAIN = 4.0

CHUNK = 8
UNROLL = 4
STEP = 16
LEAD = 8
LAST = 16


def neuron_traces(spikes, stp_init, trace_init):
    fired = spikes.astype(jnp.float32)
    use_level, supply = stp_init[0], stp_init[1]
    pre_fast, post_fast, post_slow = trace_init[0], trace_init[1], trace_init[2]
    rows = []
    for step in range(spikes.shape[0]):
        s = fired[step]
        use_level = BASE_USE + (use_level - BASE_USE) * USE_DECAY
        use_level = use_level + s * BASE_USE * (1.0 - use_level)
        release = s * use_level * supply
        supply = supply + SUPPLY_RATE * (1.0 - supply) - release
        pre_fast = pre_fast * PLUS_DECAY + s
        potent = s * (PAIR_UP + TRIPLET_UP * post_slow)
        depress = PAIR_DOWN * post_fast
        post_fast = post_fast * MINUS_DECAY + s
        post_slow = post_slow * SLOW_DECAY + s
        rows.append((release, pre_fast, potent, depress))
    return [jnp.stack([row[n] for row in rows]) for n in range(4)]


def split(x):
    high = x.astype(jnp.bfloat16).astype(jnp.float32)
    return high, x - high


def updated(block, post, pre):
    change = jnp.dot(post, pre, preferred_element_type=jnp.float32)
    return jnp.clip(block + change, 0.0, WEIGHT_MAX)


def own_kernel(steps, rows, cols, n_pieces):
    stride = -(-2 * steps // 8) * 8
    lo_row = -(-steps // 8) * 8

    def kernel(*refs):
        info, pre_ids, post_ids = refs[:3]
        pieces = refs[3:3 + n_pieces]
        posts, far_posts, weights = refs[3 + n_pieces:6 + n_pieces]
        out, current, pre_out, far_out = refs[6 + n_pieces:10 + n_pieces]
        buf, work, rel, post_t, acc, in_sem, out_sem = refs[10 + n_pieces:]
        group = buf.shape[-1]
        half_chunks = out.shape[0] // CHUNK
        filled, row, col = info[0], info[1], info[2]
        chunks = (filled + CHUNK - 1) // CHUNK
        kept = jnp.minimum(chunks, half_chunks)

        def fetch(i):
            at = pl.ds(i * CHUNK, CHUNK)
            return pltpu.make_async_copy(weights.at[at], buf.at[at], in_sem.at[i])

        def store(i):
            at = pl.ds(i * CHUNK, CHUNK)
            return pltpu.make_async_copy(buf.at[at], out.at[at], out_sem.at[i])

        @pl.loop(0, chunks)
        def _(i):
            fetch(i).start()

        work[...] = jnp.zeros_like(work)
        lane = lax.broadcasted_iota(jnp.int32, (steps, group), 1)
        polarity = jnp.where(lane % 5 == 4, -INHIB_GAIN, 1.0).astype(jnp.float32)
        at = 0
        for piece in pieces:
            for k in range(piece.shape[0]):
                high, low = split(piece[k])
                work[0:2 * steps] = high
                work[stride:stride + 2 * steps] = low
                work[2 * stride:2 * stride + 2 * steps] = high
                pre_out[at] = work[...].astype(jnp.bfloat16)
                at += 1
        for j in range(cols):
            for source, target in ((posts, post_t), (far_posts, far_out)):
                high, low = split(source[j])
                work[0:2 * steps] = high
                work[stride:stride + 2 * steps] = high
                work[2 * stride:2 * stride + 2 * steps] = low
                target[j] = work[...].T.astype(jnp.bfloat16)
        work[...] = jnp.zeros_like(work)
        at = 0
        for piece in pieces:
            for k in range(piece.shape[0]):
                high, low = split(piece[k, steps:2 * steps] * polarity)
                work[0:steps] = high
                work[lo_row:lo_row + steps] = low
                turned = work[...].T.astype(jnp.bfloat16)
                rel[at, 0:group] = turned
                rel[at, group:2 * group] = turned
                at += 1
        acc[...] = jnp.zeros_like(acc)

        def slot(s, keep):
            block = buf[s]
            p = pre_ids[s] ^ row
            q = post_ids[s] ^ col
            high = block.astype(jnp.bfloat16)
            low = (block - high.astype(jnp.float32)).astype(jnp.bfloat16)
            both = jnp.concatenate([high, low], axis=1)
            flow = jnp.dot(both, rel[p], preferred_element_type=jnp.float32)
            bin_at = jnp.where(s < filled, q, cols)
            acc[bin_at] = acc[bin_at] + flow
            if keep:
                buf[s] = updated(block, post_t[q], pre_out[p])

        @pl.loop(0, kept)
        def _(i):
            fetch(i).wait()

            @pl.loop(i * CHUNK, (i + 1) * CHUNK, step=UNROLL)
            def _(s):
                for n in range(UNROLL):
                    slot(s + n, True)

            store(i).start()

        @pl.loop(kept, chunks)
        def _(i):
            fetch(i).wait()

            @pl.loop(i * CHUNK, (i + 1) * CHUNK, step=UNROLL)
            def _(s):
                for n in range(UNROLL):
                    slot(s + n, False)

        for j in range(cols):
            turned = acc[j].T
            current[j] = turned[0:steps] + turned[lo_row:lo_row + steps]

        @pl.loop(0, kept)
        def _(i):
            store(i).wait()

    return kernel


def own_work(info, pre_ids, post_ids, pieces, posts, far_posts, weights):
    slots, group = weights.shape[0], weights.shape[-1]
    half = slots // 2
    cols, steps = posts.shape[0], posts.shape[1] // 2
    rows = sum(piece.shape[0] for piece in pieces)
    smem = pl.BlockSpec(memory_space=pltpu.SMEM)
    vmem = pl.BlockSpec(memory_space=pltpu.VMEM)
    hbm = pl.BlockSpec(memory_space=pl.ANY)
    square = (group, group)
    return pl.pallas_call(
        own_kernel(steps, rows, cols, len(pieces)),
        out_shape=(
            jax.ShapeDtypeStruct((half,) + square, jnp.float32),
            jax.ShapeDtypeStruct((cols, steps, group), jnp.float32),
            jax.ShapeDtypeStruct((rows,) + square, jnp.bfloat16),
            jax.ShapeDtypeStruct((cols,) + square, jnp.bfloat16),
        ),
        in_specs=[smem] * 3 + [vmem] * (len(pieces) + 2) + [hbm],
        out_specs=(hbm, vmem, vmem, vmem),
        scratch_shapes=[
            pltpu.VMEM((slots,) + square, jnp.float32),
            pltpu.VMEM(square, jnp.float32),
            pltpu.VMEM((rows, 2 * group, group), jnp.bfloat16),
            pltpu.VMEM((cols,) + square, jnp.bfloat16),
            pltpu.VMEM((cols + 1,) + square, jnp.float32),
            pltpu.SemaphoreType.DMA((slots // CHUNK,)),
            pltpu.SemaphoreType.DMA((half // CHUNK,)),
        ],
        cost_estimate=pl.CostEstimate(flops=10**9, bytes_accessed=2 * 10**7, transcendentals=0),
        name="own_slots",
    )(info, pre_ids, post_ids, *pieces, posts, far_posts, weights)


def received_kernel(info, ids, pre_table, post_table, blocks, _, out, buf, in_sem, out_sem):
    first, moved, row, col, place = info[0], info[1], info[2], info[3], info[4]
    size = blocks.shape[0]
    count = jnp.clip(moved - first, 0, size)

    def fetch(i):
        at = pl.ds(i * CHUNK, CHUNK)
        return pltpu.make_async_copy(blocks.at[at], buf.at[at], in_sem.at[i])

    def store(j):
        return pltpu.make_async_copy(buf.at[j], out.at[place + first + j], out_sem.at[j])

    @pl.loop(0, (count + CHUNK - 1) // CHUNK)
    def _(i):
        fetch(i).start()

    @pl.loop(0, (count + CHUNK - 1) // CHUNK)
    def _(i):
        fetch(i).wait()

        @pl.loop(i * CHUNK, (i + 1) * CHUNK, step=UNROLL)
        def _(s):
            for n in range(UNROLL):
                j = s + n
                p = ids[0, first + j] ^ row
                q = ids[1, first + j] ^ col
                buf[j] = updated(buf[j], post_table[q], pre_table[p])

        @pl.loop(i * CHUNK, jnp.minimum(i * CHUNK + CHUNK, count))
        def _(j):
            store(j).start()

    @pl.loop(0, count)
    def _(j):
        store(j).wait()


def received_work(info, ids, pre_table, post_table, blocks, out):
    smem = pl.BlockSpec(memory_space=pltpu.SMEM)
    vmem = pl.BlockSpec(memory_space=pltpu.VMEM)
    hbm = pl.BlockSpec(memory_space=pl.ANY)
    size = blocks.shape[0]
    return pl.pallas_call(
        received_kernel,
        out_shape=jax.ShapeDtypeStruct(out.shape, out.dtype),
        in_specs=[smem, smem, vmem, vmem, hbm, hbm],
        out_specs=hbm,
        scratch_shapes=[
            pltpu.VMEM(blocks.shape, jnp.float32),
            pltpu.SemaphoreType.DMA((size // CHUNK,)),
            pltpu.SemaphoreType.DMA((size,)),
        ],
        input_output_aliases={5: 0},
        cost_estimate=pl.CostEstimate(
            flops=2 * 10**6 * size, bytes_accessed=2**17 * size, transcendentals=0
        ),
        name="received_slots",
    )(info, ids, pre_table, post_table, blocks, out)


def swap(value, axis, mask):
    return lax.ppermute(value, axis, [(n, n ^ mask) for n in range(lax.axis_size(axis))])


def body(spikes, stp_init, trace_init, weights, block_pre, block_post, block_count):
    group = weights.shape[-1]
    half = weights.shape[2] // 2
    steps = spikes.shape[0]
    rows = lax.axis_size("row")
    cols = lax.axis_size("col")
    far = rows // 2
    row = lax.axis_index("row").astype(jnp.int32)
    col = lax.axis_index("col").astype(jnp.int32)
    own_blocks = weights[0, 0]
    pre_ids = block_pre[0, 0]
    post_ids = block_post[0, 0]
    filled = block_count[0, 0]

    far_ids = swap(jnp.stack([pre_ids[half:], post_ids[half:]]), "row", far)
    release, pre_fast, potent, depress = neuron_traces(spikes, stp_init, trace_init)
    pre_rows = jnp.concatenate([pre_fast, release])[None]
    post_rows = jnp.concatenate([LEARN_RATE * potent, -LEARN_RATE * depress])[None]
    posts = jnp.concatenate([post_rows] + [swap(post_rows, "col", m) for m in range(1, cols)])
    near = jnp.concatenate([pre_rows, swap(pre_rows, "row", 1)])
    pieces = [near]
    for m in range(2, rows, 2):
        if m == far:
            got = swap(jnp.concatenate([near, posts]), "row", m)
            pieces.append(got[:2])
            far_posts = got[2:]
        else:
            pieces.append(swap(near, "row", m))

    moved = jnp.abs(filled - half)
    sending = filled > half
    upward = sending == (row < far)
    info = jnp.stack([filled, row, col])
    arriving = jnp.where(sending, 0, moved)
    steps_needed = (moved + STEP - 1) // STEP
    branch_count = half // STEP
    choice = jnp.where(upward | (moved == 0), steps_needed, branch_count + steps_needed)
    up_pairs = [(n, n + far) for n in range(far)]
    down_pairs = [(n + far, n) for n in range(far)]

    def branch(size, pairs):
        def run(*operands):
            info, pre_ids, post_ids, far_ids, arriving, posts, far_posts, blocks, *pieces = operands
            cuts = [0]
            if size > LEAD + LAST:
                cuts += [LEAD, size - LAST]
            elif size > 0:
                cuts += [size // 2]
            cuts.append(size)
            parts = []
            for a, b in zip(cuts[:-1], cuts[1:]):
                if b > a:
                    parts.append((a, lax.ppermute(blocks[half + a:half + b], "row", pairs)))
            out, current, pre_table, far_table = own_work(
                info, pre_ids, post_ids, pieces, posts, far_posts, blocks
            )
            for a, part in parts:
                got_info = jnp.stack([jnp.int32(a), arriving, info[1], info[2], info[0]])
                out = received_work(got_info, far_ids, pre_table, far_table, part, out)
            return out, current
        return run

    branches = [branch(n * STEP, up_pairs) for n in range(branch_count + 1)]
    branches += [branch(n * STEP, down_pairs) for n in range(1, branch_count + 1)]
    new_blocks, current = lax.switch(
        choice, branches,
        info, pre_ids, post_ids, far_ids, arriving, posts, far_posts, own_blocks, *pieces,
    )
    drive = current[0]
    for m in range(1, cols):
        drive = drive + swap(current[m], "col", m)
    gain = 1.0 / math.sqrt(group * half)
    state = jnp.zeros_like(drive[0])
    filtered = []
    for step in range(steps):
        state = state * SYN_DECAY + gain * drive[step]
        filtered.append(state)
    return (new_blocks[None, None], jnp.stack(filtered))


def solution(mesh):
    placed = (
        P(None, ("row", "col")),
        P(None, ("row", "col")),
        P(None, ("row", "col")),
        P("row", "col", None, None, None),
        P("row", "col", None),
        P("row", "col", None),
        P("row", "col"),
    )
    return jax.shard_map(
        body,
        mesh=mesh,
        in_specs=placed,
        out_specs=(P("row", "col", None, None, None), P(None, ("row", "col"))),
        check_vma=False,
    )
```

```python
import math

import jax
import jax.numpy as jnp
from jax import lax
from jax.experimental import pallas as pl
from jax.experimental.pallas import tpu as pltpu
from jax.sharding import PartitionSpec as P


BASE_USE = 0.25
USE_DECAY = 0.98
SUPPLY_RATE = 0.005
PLUS_DECAY = math.exp(-1.0 / 16.8)
MINUS_DECAY = math.exp(-1.0 / 33.7)
SLOW_DECAY = math.exp(-1.0 / 114.0)
SYN_DECAY = math.exp(-1.0 / 5.0)
PAIR_UP = 1.0
TRIPLET_UP = 0.8
PAIR_DOWN = 0.9
LEARN_RATE = 0.02
WEIGHT_MAX = 1.0
INHIB_GAIN = 4.0

CHUNK = 8
UNROLL = 4
FEW = 2
LEAD = 8
LAST = 16


def traces_kernel(spikes, stp_init, trace_init, pre_rows, post_rows):
    steps = spikes.shape[0]
    use_level, supply = stp_init[0:1], stp_init[1:2]
    pre_fast, post_fast, post_slow = trace_init[0:1], trace_init[1:2], trace_init[2:3]
    for t in range(steps):
        s = spikes[t:t + 1].astype(jnp.float32)
        use_level = BASE_USE + (use_level - BASE_USE) * USE_DECAY
        use_level = use_level + s * BASE_USE * (1.0 - use_level)
        release = s * use_level * supply
        supply = supply + SUPPLY_RATE * (1.0 - supply) - release
        pre_fast = pre_fast * PLUS_DECAY + s
        pre_rows[0, t:t + 1] = pre_fast
        pre_rows[0, steps + t:steps + t + 1] = release
        post_rows[0, t:t + 1] = LEARN_RATE * (s * (PAIR_UP + TRIPLET_UP * post_slow))
        post_rows[0, steps + t:steps + t + 1] = -LEARN_RATE * (PAIR_DOWN * post_fast)
        post_fast = post_fast * MINUS_DECAY + s
        post_slow = post_slow * SLOW_DECAY + s


def neuron_traces(spikes, stp_init, trace_init):
    steps, group = spikes.shape
    rows = jax.ShapeDtypeStruct((1, 2 * steps, group), jnp.float32)
    return pl.pallas_call(traces_kernel, out_shape=(rows, rows), name="traces")(
        spikes, stp_init, trace_init
    )


def split(x):
    high = x.astype(jnp.bfloat16).astype(jnp.float32)
    return high, x - high


def updated(block, post, pre):
    change = jnp.dot(post, pre, preferred_element_type=jnp.float32)
    return jnp.clip(block + change, 0.0, WEIGHT_MAX)


def own_kernel(steps, rows, cols, n_pieces):
    stride = -(-2 * steps // 8) * 8
    lo_row = -(-steps // 8) * 8

    def kernel(*refs):
        info, pre_ids, post_ids = refs[:3]
        pieces = refs[3:3 + n_pieces]
        posts, far_posts, weights = refs[3 + n_pieces:6 + n_pieces]
        out, current, pre_out, far_out = refs[6 + n_pieces:10 + n_pieces]
        buf, work, raw_pre, rel, post_t, acc, in_sem, out_sem = refs[10 + n_pieces:]
        group = buf.shape[-1]
        half_chunks = out.shape[0] // CHUNK
        filled, row, col = info[0], info[1], info[2]
        chunks = (filled + CHUNK - 1) // CHUNK
        kept = jnp.minimum(chunks, half_chunks)

        def fetch(i):
            at = pl.ds(i * CHUNK, CHUNK)
            return pltpu.make_async_copy(weights.at[at], buf.at[at], in_sem.at[i])

        def store(i):
            at = pl.ds(i * CHUNK, CHUNK)
            return pltpu.make_async_copy(buf.at[at], out.at[at], out_sem.at[i])

        @pl.loop(0, chunks)
        def _(i):
            fetch(i).start()

        at = 0
        for piece in pieces:
            for k in range(piece.shape[0]):
                raw_pre[at] = piece[k]
                at += 1
        work[...] = jnp.zeros_like(work)

        def spread(value, second, third):
            high, low = split(value)
            pick = (high, low)
            work[0:2 * steps] = high
            work[stride:stride + 2 * steps] = pick[second]
            work[2 * stride:2 * stride + 2 * steps] = pick[third]

        @pl.loop(0, rows)
        def _(k):
            spread(raw_pre[k], 1, 0)
            pre_out[k] = work[...].astype(jnp.bfloat16)

        @pl.loop(0, cols)
        def _(k):
            spread(posts[k], 0, 1)
            post_t[k] = work[...].T.astype(jnp.bfloat16)
            spread(far_posts[k], 0, 1)
            far_out[k] = work[...].T.astype(jnp.bfloat16)

        work[...] = jnp.zeros_like(work)
        lane = lax.broadcasted_iota(jnp.int32, (steps, group), 1)
        polarity = jnp.where(lane % 5 == 4, -INHIB_GAIN, 1.0).astype(jnp.float32)

        @pl.loop(0, rows)
        def _(k):
            high, low = split(raw_pre[k, steps:2 * steps] * polarity)
            work[0:steps] = high
            work[lo_row:lo_row + steps] = low
            turned = work[...].T.astype(jnp.bfloat16)
            rel[k, 0:group] = turned
            rel[k, group:2 * group] = turned

        acc[...] = jnp.zeros_like(acc)

        def slot(s):
            block = buf[s]
            p = pre_ids[s] ^ row
            q = post_ids[s] ^ col
            high = block.astype(jnp.bfloat16)
            low = (block - high.astype(jnp.float32)).astype(jnp.bfloat16)
            both = jnp.concatenate([high, low], axis=1)
            flow = jnp.dot(both, rel[p], preferred_element_type=jnp.float32)
            bin_at = jnp.where(s < filled, q, cols)
            acc[bin_at] = acc[bin_at] + flow
            buf[s] = updated(block, post_t[q], pre_out[p])

        @pl.loop(0, chunks)
        def _(i):
            fetch(i).wait()

            @pl.loop(i * CHUNK, (i + 1) * CHUNK, step=UNROLL)
            def _(s):
                for n in range(UNROLL):
                    slot(s + n)

            @pl.when(i < kept)
            def _():
                store(i).start()

        @pl.loop(0, cols)
        def _(j):
            work[...] = acc[j].T
            current[j] = work[0:steps] + work[lo_row:lo_row + steps]

        @pl.loop(0, kept)
        def _(i):
            store(i).wait()

    return kernel


def own_work(info, pre_ids, post_ids, pieces, posts, far_posts, weights):
    slots, group = weights.shape[0], weights.shape[-1]
    half = slots // 2
    cols, steps = posts.shape[0], posts.shape[1] // 2
    rows = sum(piece.shape[0] for piece in pieces)
    smem = pl.BlockSpec(memory_space=pltpu.SMEM)
    vmem = pl.BlockSpec(memory_space=pltpu.VMEM)
    hbm = pl.BlockSpec(memory_space=pl.ANY)
    square = (group, group)
    return pl.pallas_call(
        own_kernel(steps, rows, cols, len(pieces)),
        out_shape=(
            jax.ShapeDtypeStruct((half,) + square, jnp.float32),
            jax.ShapeDtypeStruct((cols, steps, group), jnp.float32),
            jax.ShapeDtypeStruct((rows,) + square, jnp.bfloat16),
            jax.ShapeDtypeStruct((cols,) + square, jnp.bfloat16),
        ),
        in_specs=[smem] * 3 + [vmem] * (len(pieces) + 2) + [hbm],
        out_specs=(hbm, vmem, vmem, vmem),
        scratch_shapes=[
            pltpu.VMEM((slots,) + square, jnp.float32),
            pltpu.VMEM(square, jnp.float32),
            pltpu.VMEM((rows, 2 * steps, group), jnp.float32),
            pltpu.VMEM((rows, 2 * group, group), jnp.bfloat16),
            pltpu.VMEM((cols,) + square, jnp.bfloat16),
            pltpu.VMEM((cols + 1,) + square, jnp.float32),
            pltpu.SemaphoreType.DMA((slots // CHUNK,)),
            pltpu.SemaphoreType.DMA((half // CHUNK,)),
        ],
        cost_estimate=pl.CostEstimate(flops=10**9, bytes_accessed=2 * 10**7, transcendentals=0),
        name="own_slots",
    )(info, pre_ids, post_ids, *pieces, posts, far_posts, weights)


def received_kernel(first):
    def kernel(info, ids, pre_table, post_table, blocks, _, out, buf, in_sem, out_sem, tail_sem):
        place, row, col, moved = info[0], info[1], info[2], info[3]
        size = blocks.shape[0]
        count = jnp.clip(moved - first, 0, size)
        chunks = (count + CHUNK - 1) // CHUNK
        whole = count // CHUNK

        def fetch(i):
            at = pl.ds(i * CHUNK, CHUNK)
            return pltpu.make_async_copy(blocks.at[at], buf.at[at], in_sem.at[i])

        def store(i):
            at = pl.ds(i * CHUNK, CHUNK)
            to = pl.ds(place + first + i * CHUNK, CHUNK)
            return pltpu.make_async_copy(buf.at[at], out.at[to], out_sem.at[i])

        def store_one(j):
            to = out.at[place + first + j]
            return pltpu.make_async_copy(buf.at[j], to, tail_sem.at[j - whole * CHUNK])

        @pl.loop(0, chunks)
        def _(i):
            fetch(i).start()

        @pl.loop(0, chunks)
        def _(i):
            fetch(i).wait()

            @pl.loop(i * CHUNK, (i + 1) * CHUNK, step=FEW)
            def _(s):
                for n in range(FEW):
                    j = s + n
                    p = ids[0, first + j] ^ row
                    q = ids[1, first + j] ^ col
                    buf[j] = updated(buf[j], post_table[q], pre_table[p])

            @pl.when(i < whole)
            def _():
                store(i).start()

        @pl.loop(whole * CHUNK, count)
        def _(j):
            store_one(j).start()

        @pl.loop(0, whole)
        def _(i):
            store(i).wait()

        @pl.loop(whole * CHUNK, count)
        def _(j):
            store_one(j).wait()

    return kernel


def received_work(first, info, ids, pre_table, post_table, blocks, out):
    smem = pl.BlockSpec(memory_space=pltpu.SMEM)
    vmem = pl.BlockSpec(memory_space=pltpu.VMEM)
    hbm = pl.BlockSpec(memory_space=pl.ANY)
    size = blocks.shape[0]
    return pl.pallas_call(
        received_kernel(first),
        out_shape=jax.ShapeDtypeStruct(out.shape, out.dtype),
        in_specs=[smem, smem, vmem, vmem, hbm, hbm],
        out_specs=hbm,
        scratch_shapes=[
            pltpu.VMEM(blocks.shape, jnp.float32),
            pltpu.SemaphoreType.DMA((size // CHUNK,)),
            pltpu.SemaphoreType.DMA((size // CHUNK,)),
            pltpu.SemaphoreType.DMA((CHUNK,)),
        ],
        input_output_aliases={5: 0},
        cost_estimate=pl.CostEstimate(
            flops=2 * 10**6 * size, bytes_accessed=2**17 * size, transcendentals=0
        ),
        name="received_slots",
    )(info, ids, pre_table, post_table, blocks, out)


def swap(value, axis, mask):
    return lax.ppermute(value, axis, [(n, n ^ mask) for n in range(lax.axis_size(axis))])


def body(spikes, stp_init, trace_init, weights, block_pre, block_post, block_count):
    group = weights.shape[-1]
    half = weights.shape[2] // 2
    steps = spikes.shape[0]
    rows = lax.axis_size("row")
    cols = lax.axis_size("col")
    far = rows // 2
    row = lax.axis_index("row").astype(jnp.int32)
    col = lax.axis_index("col").astype(jnp.int32)
    own_blocks = weights[0, 0]
    pre_ids = block_pre[0, 0]
    post_ids = block_post[0, 0]
    filled = block_count[0, 0]

    far_ids = swap(jnp.stack([pre_ids[half:], post_ids[half:]]), "row", far)
    pre_rows, post_rows = neuron_traces(spikes, stp_init, trace_init)
    posts = jnp.concatenate([post_rows] + [swap(post_rows, "col", m) for m in range(1, cols)])
    near = jnp.concatenate([pre_rows, swap(pre_rows, "row", 1)])
    pieces = [near]
    for m in range(2, rows, 2):
        if m == far:
            got = swap(jnp.concatenate([near, posts]), "row", m)
            pieces.append(got[:2])
            far_posts = got[2:]
        else:
            pieces.append(swap(near, "row", m))

    moved = jnp.abs(filled - half)
    sending = filled > half
    upward = sending == (row < far)
    info = jnp.stack([filled, row, col, jnp.where(sending, 0, moved)])
    quarter = half // 4
    sizes = list(range(CHUNK, quarter, CHUNK)) + list(range(quarter, half + 1, 2 * CHUNK))
    sizes = sizes[::-1]
    kind = sum((moved <= size).astype(jnp.int32) for size in sizes)
    choice = jnp.where(moved == 0, 2 * len(sizes), 2 * (kind - 1) + upward.astype(jnp.int32))
    up_pairs = [(n, n + far) for n in range(far)]
    down_pairs = [(n + far, n) for n in range(far)]

    def branch(size, pairs):
        def run(info, pre_ids, post_ids, far_ids, posts, far_posts, blocks, *pieces):
            if size > half // 2 + LAST:
                cuts = [0, LEAD, size - LAST, size]
            elif size > quarter:
                cuts = [0, LEAD, size]
            else:
                cuts = [0, size][:size + 1]
            parts = []
            for a, b in zip(cuts[:-1], cuts[1:]):
                part = blocks[half + a:half + b]
                parts.append((a, lax.ppermute(part, "row", pairs)))
            out, current, pre_table, far_table = own_work(
                info, pre_ids, post_ids, pieces, posts, far_posts, blocks
            )
            for a, part in parts:
                out = received_work(a, info, far_ids, pre_table, far_table, part, out)
            return out, current

        return run

    branches = []
    for size in sizes:
        branches += [branch(size, down_pairs), branch(size, up_pairs)]
    branches.append(branch(0, up_pairs))
    new_blocks, current = lax.switch(
        choice, branches,
        info, pre_ids, post_ids, far_ids, posts, far_posts, own_blocks, *pieces,
    )
    drive = current[0]
    for m in range(1, cols):
        drive = drive + swap(current[m], "col", m)
    gain = 1.0 / math.sqrt(group * half)
    state = jnp.zeros_like(drive[0])
    filtered = []
    for step in range(steps):
        state = state * SYN_DECAY + gain * drive[step]
        filtered.append(state)
    return (new_blocks[None, None], jnp.stack(filtered))


def solution(mesh):
    placed = (
        P(None, ("row", "col")),
        P(None, ("row", "col")),
        P(None, ("row", "col")),
        P("row", "col", None, None, None),
        P("row", "col", None),
        P("row", "col", None),
        P("row", "col"),
    )
    return jax.shard_map(
        body,
        mesh=mesh,
        in_specs=placed,
        out_specs=(P("row", "col", None, None, None), P(None, ("row", "col"))),
        check_vma=False,
    )
```

```python
import math

import jax
import jax.numpy as jnp
from jax import lax
from jax.experimental import pallas as pl
from jax.experimental.pallas import tpu as pltpu
from jax.sharding import PartitionSpec as P


BASE_USE = 0.25
USE_DECAY = 0.98
SUPPLY_RATE = 0.005
PLUS_DECAY = math.exp(-1.0 / 16.8)
MINUS_DECAY = math.exp(-1.0 / 33.7)
SLOW_DECAY = math.exp(-1.0 / 114.0)
SYN_DECAY = math.exp(-1.0 / 5.0)
PAIR_UP = 1.0
TRIPLET_UP = 0.8
PAIR_DOWN = 0.9
LEARN_RATE = 0.02
WEIGHT_MAX = 1.0
INHIB_GAIN = 4.0

CHUNK = 8
UNROLL = 4
FEW = 4
LEAD = 8
LAST = 8


def traces_kernel(spikes, stp_init, trace_init, pre_rows, post_rows):
    steps = spikes.shape[0]
    use_level, supply = stp_init[0:1], stp_init[1:2]
    pre_fast, post_fast, post_slow = trace_init[0:1], trace_init[1:2], trace_init[2:3]
    for t in range(steps):
        s = spikes[t:t + 1].astype(jnp.float32)
        use_level = BASE_USE + (use_level - BASE_USE) * USE_DECAY
        use_level = use_level + s * BASE_USE * (1.0 - use_level)
        release = s * use_level * supply
        supply = supply + SUPPLY_RATE * (1.0 - supply) - release
        pre_fast = pre_fast * PLUS_DECAY + s
        pre_rows[0, t:t + 1] = pre_fast
        pre_rows[0, steps + t:steps + t + 1] = release
        post_rows[0, t:t + 1] = LEARN_RATE * (s * (PAIR_UP + TRIPLET_UP * post_slow))
        post_rows[0, steps + t:steps + t + 1] = -LEARN_RATE * (PAIR_DOWN * post_fast)
        post_fast = post_fast * MINUS_DECAY + s
        post_slow = post_slow * SLOW_DECAY + s


def neuron_traces(spikes, stp_init, trace_init):
    steps, group = spikes.shape
    rows = jax.ShapeDtypeStruct((1, 2 * steps, group), jnp.float32)
    return pl.pallas_call(traces_kernel, out_shape=(rows, rows), name="traces")(
        spikes, stp_init, trace_init
    )


def split(x):
    high = x.astype(jnp.bfloat16).astype(jnp.float32)
    return high, x - high


def updated(block, post, pre):
    change = jnp.dot(post, pre, preferred_element_type=jnp.float32)
    return jnp.clip(block + change, 0.0, WEIGHT_MAX)


def own_kernel(steps, rows, cols, n_pieces):
    stride = -(-2 * steps // 8) * 8
    lo_row = -(-steps // 8) * 8

    def kernel(*refs):
        info, pre_ids, post_ids = refs[:3]
        pieces = refs[3:3 + n_pieces]
        posts, far_posts, weights = refs[3 + n_pieces:6 + n_pieces]
        out, current, pre_out, far_out = refs[6 + n_pieces:10 + n_pieces]
        buf, work, raw_pre, rel, post_t, acc, in_sem, out_sem = refs[10 + n_pieces:]
        group = buf.shape[-1]
        half_chunks = out.shape[0] // CHUNK
        filled, row, col = info[0], info[1], info[2]
        chunks = (filled + CHUNK - 1) // CHUNK
        kept = jnp.minimum(chunks, half_chunks)

        def fetch(i):
            at = pl.ds(i * CHUNK, CHUNK)
            return pltpu.make_async_copy(weights.at[at], buf.at[at], in_sem.at[i])

        def store(i):
            at = pl.ds(i * CHUNK, CHUNK)
            return pltpu.make_async_copy(buf.at[at], out.at[at], out_sem.at[i])

        @pl.loop(0, chunks)
        def _(i):
            fetch(i).start()

        at = 0
        for piece in pieces:
            for k in range(piece.shape[0]):
                raw_pre[at] = piece[k]
                at += 1
        work[...] = jnp.zeros_like(work)

        def spread(value, second, third):
            high, low = split(value)
            pick = (high, low)
            work[0:2 * steps] = high
            work[stride:stride + 2 * steps] = pick[second]
            work[2 * stride:2 * stride + 2 * steps] = pick[third]

        @pl.loop(0, rows)
        def _(k):
            spread(raw_pre[k], 1, 0)
            pre_out[k] = work[...].astype(jnp.bfloat16)

        @pl.loop(0, cols)
        def _(k):
            spread(posts[k], 0, 1)
            post_t[k] = work[...].T.astype(jnp.bfloat16)
            spread(far_posts[k], 0, 1)
            far_out[k] = work[...].T.astype(jnp.bfloat16)

        work[...] = jnp.zeros_like(work)
        lane = lax.broadcasted_iota(jnp.int32, (steps, group), 1)
        polarity = jnp.where(lane % 5 == 4, -INHIB_GAIN, 1.0).astype(jnp.float32)

        @pl.loop(0, rows)
        def _(k):
            high, low = split(raw_pre[k, steps:2 * steps] * polarity)
            work[0:steps] = high
            work[lo_row:lo_row + steps] = low
            turned = work[...].T.astype(jnp.bfloat16)
            rel[k, 0:group] = turned
            rel[k, group:2 * group] = turned

        acc[...] = jnp.zeros_like(acc)

        def slot(s):
            block = buf[s]
            p = pre_ids[s] ^ row
            q = post_ids[s] ^ col
            high = block.astype(jnp.bfloat16)
            low = (block - high.astype(jnp.float32)).astype(jnp.bfloat16)
            both = jnp.concatenate([high, low], axis=1)
            flow = jnp.dot(both, rel[p], preferred_element_type=jnp.float32)
            bin_at = jnp.where(s < filled, q, cols)
            acc[bin_at] = acc[bin_at] + flow
            buf[s] = updated(block, post_t[q], pre_out[p])

        @pl.loop(0, chunks)
        def _(i):
            fetch(i).wait()

            @pl.loop(i * CHUNK, (i + 1) * CHUNK, step=UNROLL)
            def _(s):
                for n in range(UNROLL):
                    slot(s + n)

            @pl.when(i < kept)
            def _():
                store(i).start()

        @pl.loop(0, cols)
        def _(j):
            work[...] = acc[j].T
            current[j] = work[0:steps] + work[lo_row:lo_row + steps]

        @pl.loop(0, kept)
        def _(i):
            store(i).wait()

    return kernel


def own_work(info, pre_ids, post_ids, pieces, posts, far_posts, weights):
    slots, group = weights.shape[0], weights.shape[-1]
    half = slots // 2
    cols, steps = posts.shape[0], posts.shape[1] // 2
    rows = sum(piece.shape[0] for piece in pieces)
    smem = pl.BlockSpec(memory_space=pltpu.SMEM)
    vmem = pl.BlockSpec(memory_space=pltpu.VMEM)
    hbm = pl.BlockSpec(memory_space=pl.ANY)
    square = (group, group)
    return pl.pallas_call(
        own_kernel(steps, rows, cols, len(pieces)),
        out_shape=(
            jax.ShapeDtypeStruct((half,) + square, jnp.float32),
            jax.ShapeDtypeStruct((cols, steps, group), jnp.float32),
            jax.ShapeDtypeStruct((rows,) + square, jnp.bfloat16),
            jax.ShapeDtypeStruct((cols,) + square, jnp.bfloat16),
        ),
        in_specs=[smem] * 3 + [vmem] * (len(pieces) + 2) + [hbm],
        out_specs=(hbm, vmem, vmem, vmem),
        scratch_shapes=[
            pltpu.VMEM((slots,) + square, jnp.float32),
            pltpu.VMEM(square, jnp.float32),
            pltpu.VMEM((rows, 2 * steps, group), jnp.float32),
            pltpu.VMEM((rows, 2 * group, group), jnp.bfloat16),
            pltpu.VMEM((cols,) + square, jnp.bfloat16),
            pltpu.VMEM((cols + 1,) + square, jnp.float32),
            pltpu.SemaphoreType.DMA((slots // CHUNK,)),
            pltpu.SemaphoreType.DMA((half // CHUNK,)),
        ],
        cost_estimate=pl.CostEstimate(flops=10**9, bytes_accessed=2 * 10**7, transcendentals=0),
        name="own_slots",
    )(info, pre_ids, post_ids, *pieces, posts, far_posts, weights)


def received_kernel(first):
    def kernel(info, ids, pre_table, post_table, blocks, _, out, buf, in_sem, out_sem, tail_sem):
        place, row, col, moved = info[0], info[1], info[2], info[3]
        size = blocks.shape[0]
        count = jnp.clip(moved - first, 0, size)
        chunks = (count + CHUNK - 1) // CHUNK
        whole = count // CHUNK

        def fetch(i):
            at = pl.ds(i * CHUNK, CHUNK)
            return pltpu.make_async_copy(blocks.at[at], buf.at[at], in_sem.at[i])

        def store(i):
            at = pl.ds(i * CHUNK, CHUNK)
            to = pl.ds(place + first + i * CHUNK, CHUNK)
            return pltpu.make_async_copy(buf.at[at], out.at[to], out_sem.at[i])

        def store_one(j):
            to = out.at[place + first + j]
            return pltpu.make_async_copy(buf.at[j], to, tail_sem.at[j - whole * CHUNK])

        @pl.loop(0, chunks)
        def _(i):
            fetch(i).start()

        @pl.loop(0, chunks)
        def _(i):
            fetch(i).wait()

            @pl.loop(i * CHUNK, (i + 1) * CHUNK, step=FEW)
            def _(s):
                for n in range(FEW):
                    j = s + n
                    p = ids[0, first + j] ^ row
                    q = ids[1, first + j] ^ col
                    buf[j] = updated(buf[j], post_table[q], pre_table[p])

            @pl.when(i < whole)
            def _():
                store(i).start()

        @pl.loop(whole * CHUNK, count)
        def _(j):
            store_one(j).start()

        @pl.loop(0, whole)
        def _(i):
            store(i).wait()

        @pl.loop(whole * CHUNK, count)
        def _(j):
            store_one(j).wait()

    return kernel


def received_work(first, info, ids, pre_table, post_table, blocks, out):
    smem = pl.BlockSpec(memory_space=pltpu.SMEM)
    vmem = pl.BlockSpec(memory_space=pltpu.VMEM)
    hbm = pl.BlockSpec(memory_space=pl.ANY)
    size = blocks.shape[0]
    return pl.pallas_call(
        received_kernel(first),
        out_shape=jax.ShapeDtypeStruct(out.shape, out.dtype),
        in_specs=[smem, smem, vmem, vmem, hbm, hbm],
        out_specs=hbm,
        scratch_shapes=[
            pltpu.VMEM(blocks.shape, jnp.float32),
            pltpu.SemaphoreType.DMA((size // CHUNK,)),
            pltpu.SemaphoreType.DMA((size // CHUNK,)),
            pltpu.SemaphoreType.DMA((CHUNK,)),
        ],
        input_output_aliases={5: 0},
        cost_estimate=pl.CostEstimate(
            flops=2 * 10**6 * size, bytes_accessed=2**17 * size, transcendentals=0
        ),
        name="received_slots",
    )(info, ids, pre_table, post_table, blocks, out)


def swap(value, axis, mask):
    return lax.ppermute(value, axis, [(n, n ^ mask) for n in range(lax.axis_size(axis))])


def body(spikes, stp_init, trace_init, weights, block_pre, block_post, block_count):
    group = weights.shape[-1]
    half = weights.shape[2] // 2
    steps = spikes.shape[0]
    rows = lax.axis_size("row")
    cols = lax.axis_size("col")
    far = rows // 2
    row = lax.axis_index("row").astype(jnp.int32)
    col = lax.axis_index("col").astype(jnp.int32)
    own_blocks = weights[0, 0]
    pre_ids = block_pre[0, 0]
    post_ids = block_post[0, 0]
    filled = block_count[0, 0]

    far_ids = swap(jnp.stack([pre_ids[half:], post_ids[half:]]), "row", far)
    pre_rows, post_rows = neuron_traces(spikes, stp_init, trace_init)
    posts = jnp.concatenate([post_rows] + [swap(post_rows, "col", m) for m in range(1, cols)])
    near = jnp.concatenate([pre_rows, swap(pre_rows, "row", 1)])
    pieces = [near]
    for m in range(2, rows, 2):
        if m == far:
            got = swap(jnp.concatenate([near, posts]), "row", m)
            pieces.append(got[:2])
            far_posts = got[2:]
        else:
            pieces.append(swap(near, "row", m))

    moved = jnp.abs(filled - half)
    sending = filled > half
    upward = sending == (row < far)
    info = jnp.stack([filled, row, col, jnp.where(sending, 0, moved)])
    quarter = half // 4
    sizes = list(range(CHUNK, quarter, CHUNK)) + list(range(quarter, half + 1, 2 * CHUNK))
    sizes = sizes[::-1]
    kind = sum((moved <= size).astype(jnp.int32) for size in sizes)
    choice = jnp.where(moved == 0, 2 * len(sizes), 2 * (kind - 1) + upward.astype(jnp.int32))
    up_pairs = [(n, n + far) for n in range(far)]
    down_pairs = [(n + far, n) for n in range(far)]

    def branch(size, pairs):
        def run(info, pre_ids, post_ids, far_ids, posts, far_posts, blocks, *pieces):
            if size > half * 5 // 8:
                cuts = [0, LEAD, size - LAST, size]
            elif size > quarter:
                cuts = [0, LEAD, size]
            else:
                cuts = [0, size][:size + 1]
            parts = []
            for a, b in zip(cuts[:-1], cuts[1:]):
                part = blocks[half + a:half + b]
                parts.append((a, lax.ppermute(part, "row", pairs)))
            out, current, pre_table, far_table = own_work(
                info, pre_ids, post_ids, pieces, posts, far_posts, blocks
            )
            for a, part in parts:
                out = received_work(a, info, far_ids, pre_table, far_table, part, out)
            return out, current

        return run

    branches = []
    for size in sizes:
        branches += [branch(size, down_pairs), branch(size, up_pairs)]
    branches.append(branch(0, up_pairs))
    new_blocks, current = lax.switch(
        choice, branches,
        info, pre_ids, post_ids, far_ids, posts, far_posts, own_blocks, *pieces,
    )
    drive = current[0]
    for m in range(1, cols):
        drive = drive + swap(current[m], "col", m)
    gain = 1.0 / math.sqrt(group * half)
    state = jnp.zeros_like(drive[0])
    filtered = []
    for step in range(steps):
        state = state * SYN_DECAY + gain * drive[step]
        filtered.append(state)
    return (new_blocks[None, None], jnp.stack(filtered))


def solution(mesh):
    placed = (
        P(None, ("row", "col")),
        P(None, ("row", "col")),
        P(None, ("row", "col")),
        P("row", "col", None, None, None),
        P("row", "col", None),
        P("row", "col", None),
        P("row", "col"),
    )
    return jax.shard_map(
        body,
        mesh=mesh,
        in_specs=placed,
        out_specs=(P("row", "col", None, None, None), P(None, ("row", "col"))),
        check_vma=False,
    )
```
